32 devices in a mesh: band: 8 (over z, x), plane: 4 (over y, core).
Axes of the slice: x: 2, y: 2, z: 4, core: 2. Of those that a mesh axis runs over, the one named last changes fastest.
Arguments:
- orbitals: float32 [8, 112, 12544], P('band', 'plane'), may hold values from -6 to 6
Outputs:
- exchange_w: float32 [8, 112, 12544], P('band', 'plane')
The draws below stay inside these ranges and needn't reach their ends.
All inputs are finite; a program needn't handle non-finite values.
Results may differ from the reference program's by a relative error of at most 0.000082.
Values sent between devices are 32-bit elements; how exact they have to be, the bound alone decides.
A program may use at most 64 MiB of HBM per device.

```python
import math
import jax
import jax.numpy as jnp
from jax import lax

NG = 112
B = 1
ROUNDS = 2
ORB = 8


def block_levels(own_key, shape, pieces, least, largest):
    factor_of = 1.0
    for dim, blocks in pieces:
        steps = jax.random.uniform(jax.random.fold_in(jax.random.fold_in(own_key, 6), dim), (blocks,), jnp.float32, least / len(pieces), largest / len(pieces))
        factor_of = factor_of * jnp.repeat(jnp.exp(steps), shape[dim] // blocks).reshape((-1,) + (1,) * (len(shape) - 1 - dim))
    return factor_of


def noise(rng, dims, width, most, split=(), kind=jnp.bfloat16):
    gain = block_levels(rng, dims, split, -0.22, 0.18) if split else 1.0
    drawn = jax.random.normal(rng, dims, jnp.float32) * width * gain
    return jnp.minimum(jnp.maximum(drawn, -most), most).astype(kind)


def setup_inputs(seed: int = 0) -> dict:
    seeds = jax.random.split(jax.random.key(seed), 2)
    orbitals = noise(seeds[0], (ORB, NG, NG * NG), 1.0, 6.0, ((0, 8), (1, 4)), jnp.float32)
    return dict(orbitals=orbitals)


screen_omega = 0.106
cell_length = 46.93
mixing = 0.25


def wave_number(index, count):
    return jnp.where(2 * index < count, index, index - count)


def kernel_values(squares):
    gsquare = squares * (2.0 * math.pi / cell_length) ** 2
    safe = jnp.where(gsquare > 0, gsquare, 1.0)
    values = 4.0 * math.pi / safe * (1.0 - jnp.exp(-safe / (4.0 * screen_omega * screen_omega)))
    return jnp.where(gsquare > 0, values, math.pi / (screen_omega * screen_omega))


def reference(orbitals):
    field = orbitals.reshape(ORB, NG, NG, NG)
    sources = field[: ROUNDS * B]
    frequency = wave_number(jnp.arange(NG, dtype=jnp.int32), NG).astype(jnp.float32)
    squares = frequency[:, None, None] ** 2 + frequency[None, :, None] ** 2 + frequency[None, None, :] ** 2
    kernel = kernel_values(squares)

    def single(orbital):
        density = orbital[None] * sources
        spectrum = jnp.fft.fftn(density, axes=(1, 2, 3))
        potential = jnp.real(jnp.fft.ifftn(spectrum * kernel, axes=(1, 2, 3)))
        return -mixing * jnp.sum(sources * potential, axis=0)

    result = lax.map(single, field)
    return result.reshape(ORB, NG, NG * NG)
```

```python
import functools
import math

import jax
import jax.numpy as jnp
import numpy as np
from jax import lax
from jax.experimental import pallas as pl
from jax.experimental.pallas import tpu as pltpu
from jax.sharding import PartitionSpec as P

SOURCES = 2

screen_omega = 0.106
cell_length = 46.93
mixing = 0.25
high = lax.Precision.HIGH


def kernel_values(squares):
    gsquare = squares * (2.0 * math.pi / cell_length) ** 2
    safe = jnp.where(gsquare > 0, gsquare, 1.0)
    values = 4.0 * math.pi / safe * (1.0 - jnp.exp(-safe / (4.0 * screen_omega * screen_omega)))
    return jnp.where(gsquare > 0, values, math.pi / (screen_omega * screen_omega))


def real_basis(count):
    half = count // 2
    freq = np.array(list(range(half + 1)) + list(range(1, count - half)))
    angle = 2.0 * np.pi * (np.arange(count)[:, None] * freq[None, :] % count) / count
    table = np.where(np.arange(count)[None, :] <= half, np.cos(angle), np.sin(angle))
    table = table / np.sqrt((table**2).sum(axis=0, keepdims=True))
    return table.astype(np.float32), freq.astype(np.float32)


def spread_kernel(nband, chunks, psi_ref, src_ref, send_sem, recv_sem, own_sem):
    me = lax.axis_index("band")
    mine = lax.rem(me, SOURCES)
    partner = me + 1 - 2 * mine
    above = lax.rem(me + 2, nband)
    below = lax.rem(me + nband - 2, nband)
    size = psi_ref.shape[0] // chunks

    barrier = pltpu.get_barrier_semaphore()
    for other in (partner, above, below):
        pl.semaphore_signal(barrier, inc=1, device_id={"band": other}, device_id_type=pl.DeviceIdType.MESH)
    pl.semaphore_wait(barrier, 3)

    def part(which, c):
        return src_ref.at[which, pl.ds(c * size, size)]

    def own(c):
        return pltpu.make_async_copy(psi_ref.at[pl.ds(c * size, size)], part(mine, c), own_sem.at[c])

    def remote(kind, which, c, target):
        return pltpu.make_async_remote_copy(
            src_ref=part(which, c),
            dst_ref=part(which, c),
            send_sem=send_sem.at[kind, c],
            recv_sem=recv_sem.at[kind, c],
            device_id={"band": target},
            device_id_type=pl.DeviceIdType.MESH,
        )

    @pl.when(me < SOURCES)
    def _():
        for c in range(chunks):
            own(c).start()

    for c in range(chunks):
        @pl.when(me < SOURCES)
        def _():
            own(c).wait()

        @pl.when(me >= SOURCES)
        def _():
            remote(0, mine, c, above).wait_recv()

        @pl.when(me + 2 < nband)
        def _():
            remote(0, mine, c, above).start()

        remote(1, mine, c, partner).start()

    for c in range(chunks):
        remote(1, 1 - mine, c, partner).wait_recv()
        remote(1, mine, c, partner).wait_send()

        @pl.when(me + 2 < nband)
        def _():
            remote(0, mine, c, above).wait_send()


def spread(local):
    nband = lax.axis_size("band")
    thick = local.shape[0]
    chunks = next(c for c in (14, 7, 1) if thick % c == 0)
    return pl.pallas_call(
        functools.partial(spread_kernel, nband, chunks),
        out_shape=jax.ShapeDtypeStruct((SOURCES,) + local.shape, jnp.float32),
        in_specs=[pl.BlockSpec(memory_space=pltpu.VMEM)],
        out_specs=pl.BlockSpec(memory_space=pltpu.VMEM),
        scratch_shapes=[
            pltpu.SemaphoreType.DMA((2, chunks)),
            pltpu.SemaphoreType.DMA((2, chunks)),
            pltpu.SemaphoreType.DMA((chunks,)),
        ],
        compiler_params=pltpu.CompilerParams(collective_id=0, has_side_effects=True),
        name="spread",
    )(local)


def on_device(orbitals):
    nplane = lax.axis_size("plane")
    rows, thick, flat = orbitals.shape
    count = thick * nplane
    table, freq = real_basis(count)
    freq = jnp.asarray(freq)
    local = orbitals.reshape(rows * thick, count, count)
    freq_mine = lax.dynamic_slice(freq, (lax.axis_index("plane") * thick,), (thick,))
    kernel = kernel_values(
        freq[:, None, None] ** 2 + freq_mine[None, :, None] ** 2 + freq[None, None, :] ** 2
    )
    sources = spread(local)

    def along(spec, values):
        return jnp.einsum(spec, values, table, precision=high)

    total = 0.0
    for j in range(SOURCES):
        density = local * sources[j]
        spectrum = along("xbc,yb->xyc".replace("yb", "by"), along("xyz,zc->xyc", density))
        moved = lax.all_to_all(spectrum, "plane", split_axis=1, concat_axis=0, tiled=True)
        filtered = along("xbc,xa->abc", moved) * kernel
        back = along("abc,xa->xbc", filtered)
        back = lax.all_to_all(back, "plane", split_axis=0, concat_axis=1, tiled=True)
        potential = along("xyc,zc->xyz", along("xbc,yb->xyc", back))
        total = total + sources[j] * potential
    return (-mixing * total).reshape(rows, thick, flat)


def solution(mesh):
    placed = (P("band", "plane", None),)
    return jax.shard_map(
        on_device, mesh=mesh, in_specs=placed, out_specs=P("band", "plane", None), check_vma=False
    )
```

```python
import functools
import math

import jax
import jax.numpy as jnp
import numpy as np
from jax import lax
from jax.experimental import pallas as pl
from jax.experimental.pallas import tpu as pltpu
from jax.sharding import PartitionSpec as P

SOURCES = 2

screen_omega = 0.106
cell_length = 46.93
mixing = 0.25


def kernel_values(squares):
    gsquare = squares * (2.0 * math.pi / cell_length) ** 2
    safe = jnp.where(gsquare > 0, gsquare, 1.0)
    values = 4.0 * math.pi / safe * (1.0 - jnp.exp(-safe / (4.0 * screen_omega * screen_omega)))
    return jnp.where(gsquare > 0, values, math.pi / (screen_omega * screen_omega))


def real_basis(count):
    half = count // 2
    freq = np.array(list(range(half + 1)) + list(range(1, count - half)))
    angle = 2.0 * np.pi * (np.arange(count)[:, None] * freq[None, :] % count) / count
    table = np.where(np.arange(count)[None, :] <= half, np.cos(angle), np.sin(angle))
    table = table / np.sqrt((table**2).sum(axis=0, keepdims=True))
    return table.astype(np.float32), freq.astype(np.float32)


MESH = pl.DeviceIdType.MESH


def rounded(value, unit):
    return -(-value // unit) * unit


def high_low(table):
    high = table.astype(jnp.bfloat16)
    low = (table - high.astype(np.float32)).astype(jnp.bfloat16)
    return high, low


def right_table(table, lanes):
    count = table.shape[0]
    high, low = high_low(table)
    out = np.zeros((2 * lanes, 2 * lanes), jnp.bfloat16)
    out[:count, :count] = high
    out[lanes : lanes + count, :count] = high
    out[:count, lanes : lanes + count] = low
    return out


def left_table(table):
    return np.concatenate(high_low(table), axis=0)


def split(values):
    high = values.astype(jnp.bfloat16)
    low = (values - high.astype(jnp.float32)).astype(jnp.bfloat16)
    return jnp.concatenate([high, low], axis=-1)


def from_right(values, table):
    lanes = values.shape[-1]
    out = jnp.dot(split(values), table, preferred_element_type=jnp.float32)
    return out[:, :lanes] + out[:, lanes:]


def from_left(table, values):
    count, lanes = values.shape
    out = jnp.dot(table, split(values), preferred_element_type=jnp.float32)
    return out[:count, :lanes] + (out[:count, lanes:] + out[count:, :lanes])


def exchange_kernel(
    nband, nplane, lines, early,
    psi_ref, filter_ref, right_fwd_ref, right_inv_ref, left_fwd_ref, left_inv_ref, out_ref,
    src_ref, send_ref, full_ref, back_ref,
    spread_send, spread_recv, own_sem, fwd_send, fwd_recv, fwd_own, back_send, back_recv, back_own,
):
    me = lax.axis_index("band")
    here = lax.axis_index("plane")
    mine = lax.rem(me, SOURCES)
    partner = me + 1 - 2 * mine
    above = lax.rem(me + 2, nband)
    below = lax.rem(me + nband - 2, nband)
    thick, count, lanes = psi_ref.shape
    padded = full_ref.shape[1]

    barrier = pltpu.get_barrier_semaphore()
    for other in (partner, above, below):
        pl.semaphore_signal(barrier, inc=1, device_id={"band": other}, device_id_type=MESH)
    for step in range(1, nplane):
        pl.semaphore_signal(
            barrier, inc=1, device_id={"plane": lax.rem(here + step, nplane)}, device_id_type=MESH
        )
    pl.semaphore_wait(barrier, 2 + nplane)

    def own(c):
        return pltpu.make_async_copy(psi_ref.at[c], src_ref.at[mine, c], own_sem.at[c])

    def spread(kind, which, c, target):
        return pltpu.make_async_remote_copy(
            src_ref=src_ref.at[which, c],
            dst_ref=src_ref.at[which, c],
            send_sem=spread_send.at[kind, c],
            recv_sem=spread_recv.at[kind, c],
            device_id={"band": target},
            device_id_type=MESH,
        )

    def forward(step, c):
        target = lax.rem(here + step, nplane)
        return pltpu.make_async_remote_copy(
            src_ref=send_ref.at[c, target],
            dst_ref=full_ref.at[here * thick + c],
            send_sem=fwd_send.at[step - 1, c],
            recv_sem=fwd_recv.at[step - 1, c],
            device_id={"plane": target},
            device_id_type=MESH,
        )

    def forward_own(c):
        return pltpu.make_async_copy(
            send_ref.at[c, here], full_ref.at[here * thick + c], fwd_own.at[c]
        )

    def back_parts(c, target):
        if c is None:
            planes, rows = pl.ds(0, thick), pl.ds(0, early)
            source = full_ref.at[pl.ds(target * thick, thick), rows]
            return source, back_ref.at[planes, here, rows], thick
        rows = pl.ds(early, padded - early)
        return full_ref.at[target * thick + c, rows], back_ref.at[c, here, rows], c

    def backward(step, c):
        target = lax.rem(here + step, nplane)
        source, landing, slot = back_parts(c, target)
        return pltpu.make_async_remote_copy(
            src_ref=source,
            dst_ref=landing,
            send_sem=back_send.at[step - 1, slot],
            recv_sem=back_recv.at[step - 1, slot],
            device_id={"plane": target},
            device_id_type=MESH,
        )

    def backward_own(c):
        source, landing, slot = back_parts(c, here)
        return pltpu.make_async_copy(source, landing, back_own.at[slot])

    @pl.when(me < SOURCES)
    def _():
        @pl.loop(0, thick)
        def _(c):
            own(c).start()

    @pl.loop(0, thick)
    def _(c):
        @pl.when(me < SOURCES)
        def _():
            own(c).wait()

        @pl.when(me >= SOURCES)
        def _():
            spread(0, mine, c, above).wait_recv()

        @pl.when(me + 2 < nband)
        def _():
            spread(0, mine, c, above).start()

        spread(1, mine, c, partner).start()
        spread(1, 1 - mine, c, partner).wait_recv()

        psi = psi_ref[c]
        density = jnp.concatenate([psi * src_ref[j, c] for j in range(SOURCES)], axis=0)
        half = from_right(density, right_fwd_ref[...])
        whole = jnp.concatenate(
            [
                from_left(left_fwd_ref[...], half[j * count : (j + 1) * count])
                for j in range(SOURCES)
            ],
            axis=0,
        )
        for p in range(nplane):
            send_ref[c, p, 0:lines] = whole[p * lines : (p + 1) * lines]
        for step in range(1, nplane):
            forward(step, c).start()
        forward_own(c).start()

    @pl.loop(0, thick)
    def _(c):
        for step in range(1, nplane):
            forward(step, c).wait_recv()
        forward_own(c).wait()

    rows_ref = full_ref.reshape(nplane * thick * padded, lanes)

    def filtered(r):
        where = (pl.ds(r, count, stride=padded), slice(None))
        spectrum = from_left(left_fwd_ref[...], rows_ref[where]) * filter_ref[r]
        rows_ref[where] = from_left(left_inv_ref[...], spectrum)

    def filter_rows(start, stop):
        unroll = 4 if (stop - start) % 4 == 0 else 2 if (stop - start) % 2 == 0 else 1

        @pl.loop(0, (stop - start) // unroll)
        def _(t):
            for u in range(unroll):
                filtered(start + t * unroll + u)

    if early:
        filter_rows(0, early)
        for step in range(1, nplane):
            backward(step, None).start()
        backward_own(None).start()
    filter_rows(early, lines)

    @pl.loop(0, thick)
    def _(c):
        for step in range(1, nplane):
            backward(step, c).start()
        backward_own(c).start()

    if early:
        for step in range(1, nplane):
            backward(step, None).wait_recv()
        backward_own(None).wait()

    @pl.loop(0, thick)
    def _(c):
        for step in range(1, nplane):
            backward(step, c).wait_recv()
        backward_own(c).wait()
        whole = jnp.concatenate([back_ref[c, p, 0:lines] for p in range(nplane)], axis=0)
        half = jnp.concatenate(
            [
                from_left(left_inv_ref[...], whole[j * count : (j + 1) * count])
                for j in range(SOURCES)
            ],
            axis=0,
        )
        potential = from_right(half, right_inv_ref[...])
        total = src_ref[0, c] * potential[:count]
        for j in range(1, SOURCES):
            total = total + src_ref[j, c] * potential[j * count : (j + 1) * count]
        out_ref[c] = -mixing * total

    @pl.loop(0, thick)
    def _(c):
        spread(1, mine, c, partner).wait_send()

        @pl.when(me + 2 < nband)
        def _():
            spread(0, mine, c, above).wait_send()

        for step in range(1, nplane):
            forward(step, c).wait_send()
            backward(step, c).wait_send()

    if early:
        for step in range(1, nplane):
            backward(step, None).wait_send()


def on_device(orbitals):
    nband = lax.axis_size("band")
    nplane = lax.axis_size("plane")
    rows, thick, flat = orbitals.shape
    count = thick * nplane
    lanes = rounded(count, 128)
    lines = SOURCES * count // nplane
    padded = rounded(lines, 8)
    early = 16 if padded >= 32 else 8 if padded >= 16 else 0
    table, freq = real_basis(count)
    freq = jnp.asarray(freq)
    local = orbitals.reshape(thick, count, count)
    local = jnp.pad(local, ((0, 0), (0, 0), (0, lanes - count)))
    line = lax.axis_index("plane") * lines + jnp.arange(lines, dtype=jnp.int32)
    freq_mine = jnp.take(freq, line % count)
    freq_last = jnp.pad(freq, (0, lanes - count))
    filters = kernel_values(
        freq_mine[:, None, None] ** 2 + freq[None, :, None] ** 2 + freq_last[None, None, :] ** 2
    )
    tables = (
        right_table(table, lanes),
        right_table(table.T, lanes),
        left_table(table.T),
        left_table(table),
    )
    dma = pltpu.SemaphoreType.DMA
    vmem = pl.BlockSpec(memory_space=pltpu.VMEM)
    out = pl.pallas_call(
        functools.partial(exchange_kernel, nband, nplane, lines, early),
        out_shape=jax.ShapeDtypeStruct((thick, count, lanes), jnp.float32),
        in_specs=[vmem] * 6,
        out_specs=vmem,
        scratch_shapes=[
            pltpu.VMEM((SOURCES, thick, count, lanes), jnp.float32),
            pltpu.VMEM((thick, nplane, padded, lanes), jnp.float32),
            pltpu.VMEM((count, padded, lanes), jnp.float32),
            pltpu.VMEM((thick, nplane, padded, lanes), jnp.float32),
            dma((2, thick)),
            dma((2, thick)),
            dma((thick,)),
            dma((nplane - 1, thick)),
            dma((nplane - 1, thick)),
            dma((thick,)),
            dma((nplane - 1, thick + 1)),
            dma((nplane - 1, thick + 1)),
            dma((thick + 1,)),
        ],
        compiler_params=pltpu.CompilerParams(
            collective_id=0, has_side_effects=True, vmem_limit_bytes=48 * 2**20
        ),
        name="exchange",
    )(local, filters, *[jnp.asarray(t) for t in tables])
    return out[:, :, :count].reshape(rows, thick, flat)


def solution(mesh):
    placed = (P("band", "plane", None),)
    return jax.shard_map(
        on_device, mesh=mesh, in_specs=placed, out_specs=P("band", "plane", None), check_vma=False
    )
```

```python
import functools
import math

import jax
import jax.numpy as jnp
import numpy as np
from jax import lax
from jax.experimental import pallas as pl
from jax.experimental.pallas import tpu as pltpu
from jax.sharding import PartitionSpec as P

SOURCES = 2
AHEAD = 4

screen_omega = 0.106
cell_length = 46.93
mixing = 0.25


def kernel_values(squares):
    gsquare = squares * (2.0 * math.pi / cell_length) ** 2
    safe = jnp.where(gsquare > 0, gsquare, 1.0)
    values = 4.0 * math.pi / safe * (1.0 - jnp.exp(-safe / (4.0 * screen_omega * screen_omega)))
    return jnp.where(gsquare > 0, values, math.pi / (screen_omega * screen_omega))


def real_basis(count):
    half = count // 2
    freq = np.array(list(range(half + 1)) + list(range(1, count - half)))
    angle = 2.0 * np.pi * (np.arange(count)[:, None] * freq[None, :] % count) / count
    table = np.where(np.arange(count)[None, :] <= half, np.cos(angle), np.sin(angle))
    table = table / np.sqrt((table**2).sum(axis=0, keepdims=True))
    return table.astype(np.float32), freq.astype(np.float32)


MESH = pl.DeviceIdType.MESH


def rounded(value, unit):
    return -(-value // unit) * unit


def high_low(table):
    high = table.astype(jnp.bfloat16)
    low = (table - high.astype(np.float32)).astype(jnp.bfloat16)
    return high, low


def right_table(table, lanes):
    count = table.shape[0]
    high, low = high_low(table)
    out = np.zeros((2 * lanes, 2 * lanes), jnp.bfloat16)
    out[:count, :count] = high
    out[lanes : lanes + count, :count] = high
    out[:count, lanes : lanes + count] = low
    return out


def left_table(table):
    return np.concatenate(high_low(table), axis=0)


def split(values):
    high = values.astype(jnp.bfloat16)
    low = (values - high.astype(jnp.float32)).astype(jnp.bfloat16)
    return jnp.concatenate([high, low], axis=-1)


def from_right(values, table):
    lanes = values.shape[-1]
    out = jnp.dot(split(values), table, preferred_element_type=jnp.float32)
    return out[:, :lanes] + out[:, lanes:]


def from_left(table, values):
    count, lanes = values.shape
    out = jnp.dot(table, split(values), preferred_element_type=jnp.float32)
    return out[:count, :lanes] + (out[:count, lanes:] + out[count:, :lanes])


def exchange_kernel(
    nband, nplane, lines, early,
    psi_ref, filter_ref, right_fwd_ref, right_inv_ref, left_fwd_ref, left_inv_ref, out_ref,
    src_ref, send_ref, full_ref, back_ref,
    spread_send, spread_recv, own_sem, fwd_send, fwd_recv, fwd_own, back_send, back_recv, back_own,
):
    me = lax.axis_index("band")
    here = lax.axis_index("plane")
    mine = lax.rem(me, SOURCES)
    partner = me + 1 - 2 * mine
    above = lax.rem(me + 2, nband)
    below = lax.rem(me + nband - 2, nband)
    thick, count, lanes = psi_ref.shape
    padded = full_ref.shape[1]

    barrier = pltpu.get_barrier_semaphore()
    for other in (partner, above, below):
        pl.semaphore_signal(barrier, inc=1, device_id={"band": other}, device_id_type=MESH)
    for step in range(1, nplane):
        pl.semaphore_signal(
            barrier, inc=1, device_id={"plane": lax.rem(here + step, nplane)}, device_id_type=MESH
        )
    pl.semaphore_wait(barrier, 2 + nplane)

    def own(c):
        return pltpu.make_async_copy(psi_ref.at[c], src_ref.at[mine, c], own_sem.at[c])

    def spread(kind, which, c, target, first=False):
        return pltpu.make_async_remote_copy(
            src_ref=psi_ref.at[c] if first else src_ref.at[which, c],
            dst_ref=src_ref.at[which, c],
            send_sem=spread_send.at[kind, c],
            recv_sem=spread_recv.at[kind, c],
            device_id={"band": target},
            device_id_type=MESH,
        )

    def forward(step, c):
        target = lax.rem(here + step, nplane)
        return pltpu.make_async_remote_copy(
            src_ref=send_ref.at[c, target],
            dst_ref=full_ref.at[here * thick + c],
            send_sem=fwd_send.at[step - 1, c],
            recv_sem=fwd_recv.at[step - 1, c],
            device_id={"plane": target},
            device_id_type=MESH,
        )

    def forward_own(c):
        return pltpu.make_async_copy(
            send_ref.at[c, here], full_ref.at[here * thick + c], fwd_own.at[c]
        )

    def back_parts(c, target):
        if c is None:
            planes, rows = pl.ds(0, thick), pl.ds(0, early)
            source = full_ref.at[pl.ds(target * thick, thick), rows]
            return source, back_ref.at[planes, here, rows], thick
        rows = pl.ds(early, padded - early)
        return full_ref.at[target * thick + c, rows], back_ref.at[c, here, rows], c

    def backward(step, c):
        target = lax.rem(here + step, nplane)
        source, landing, slot = back_parts(c, target)
        return pltpu.make_async_remote_copy(
            src_ref=source,
            dst_ref=landing,
            send_sem=back_send.at[step - 1, slot],
            recv_sem=back_recv.at[step - 1, slot],
            device_id={"plane": target},
            device_id_type=MESH,
        )

    def backward_own(c):
        source, landing, slot = back_parts(c, here)
        return pltpu.make_async_copy(source, landing, back_own.at[slot])

    @pl.when(me < SOURCES)
    def _():
        @pl.loop(0, thick)
        def _(c):
            spread(0, mine, c, above, True).start()
            spread(1, mine, c, partner, True).start()
            own(c).start()

    def relay(c):
        @pl.when(me >= SOURCES)
        def _():
            spread(0, mine, c, above).wait_recv()

            @pl.when(me + 2 < nband)
            def _():
                spread(0, mine, c, above).start()

            spread(1, mine, c, partner).start()

    ahead = min(AHEAD, thick)
    for c in range(ahead):
        relay(c)

    @pl.loop(0, thick)
    def _(c):
        @pl.when(c + ahead < thick)
        def _():
            relay(c + ahead)

        @pl.when(me < SOURCES)
        def _():
            own(c).wait()

        spread(1, 1 - mine, c, partner).wait_recv()

        psi = psi_ref[c]
        density = jnp.concatenate([psi * src_ref[j, c] for j in range(SOURCES)], axis=0)
        half = from_right(density, right_fwd_ref[...])
        whole = jnp.concatenate(
            [
                from_left(left_fwd_ref[...], half[j * count : (j + 1) * count])
                for j in range(SOURCES)
            ],
            axis=0,
        )
        for p in range(nplane):
            send_ref[c, p, 0:lines] = whole[p * lines : (p + 1) * lines]
        for step in range(1, nplane):
            forward(step, c).start()
        forward_own(c).start()

    @pl.loop(0, thick)
    def _(c):
        for step in range(1, nplane):
            forward(step, c).wait_recv()
        forward_own(c).wait()

    rows_ref = full_ref.reshape(nplane * thick * padded, lanes)

    def filtered(r):
        where = (pl.ds(r, count, stride=padded), slice(None))
        spectrum = from_left(left_fwd_ref[...], rows_ref[where]) * filter_ref[r]
        rows_ref[where] = from_left(left_inv_ref[...], spectrum)

    def filter_rows(start, stop):
        unroll = 4 if (stop - start) % 4 == 0 else 2 if (stop - start) % 2 == 0 else 1

        @pl.loop(0, (stop - start) // unroll)
        def _(t):
            for u in range(unroll):
                filtered(start + t * unroll + u)

    if early:
        filter_rows(0, early)
        for step in range(1, nplane):
            backward(step, None).start()
        backward_own(None).start()
    filter_rows(early, lines)

    @pl.loop(0, thick)
    def _(c):
        for step in range(1, nplane):
            backward(step, c).start()
        backward_own(c).start()

    if early:
        for step in range(1, nplane):
            backward(step, None).wait_recv()
        backward_own(None).wait()

    @pl.loop(0, thick)
    def _(c):
        for step in range(1, nplane):
            backward(step, c).wait_recv()
        backward_own(c).wait()
        whole = jnp.concatenate([back_ref[c, p, 0:lines] for p in range(nplane)], axis=0)
        half = jnp.concatenate(
            [
                from_left(left_inv_ref[...], whole[j * count : (j + 1) * count])
                for j in range(SOURCES)
            ],
            axis=0,
        )
        potential = from_right(half, right_inv_ref[...])
        total = src_ref[0, c] * potential[:count]
        for j in range(1, SOURCES):
            total = total + src_ref[j, c] * potential[j * count : (j + 1) * count]
        out_ref[c] = -mixing * total

    @pl.loop(0, thick)
    def _(c):
        spread(1, mine, c, partner).wait_send()

        @pl.when(me + 2 < nband)
        def _():
            spread(0, mine, c, above).wait_send()

        for step in range(1, nplane):
            forward(step, c).wait_send()
            backward(step, c).wait_send()

    if early:
        for step in range(1, nplane):
            backward(step, None).wait_send()


def on_device(orbitals):
    nband = lax.axis_size("band")
    nplane = lax.axis_size("plane")
    rows, thick, flat = orbitals.shape
    count = thick * nplane
    lanes = rounded(count, 128)
    lines = SOURCES * count // nplane
    padded = rounded(lines, 8)
    early = 16 if padded >= 32 else 8 if padded >= 16 else 0
    table, freq = real_basis(count)
    freq = jnp.asarray(freq)
    local = orbitals.reshape(thick, count, count)
    local = jnp.pad(local, ((0, 0), (0, 0), (0, lanes - count)))
    line = lax.axis_index("plane") * lines + jnp.arange(lines, dtype=jnp.int32)
    freq_mine = jnp.take(freq, line % count)
    freq_last = jnp.pad(freq, (0, lanes - count))
    filters = kernel_values(
        freq_mine[:, None, None] ** 2 + freq[None, :, None] ** 2 + freq_last[None, None, :] ** 2
    )
    tables = (
        right_table(table, lanes),
        right_table(table.T, lanes),
        left_table(table.T),
        left_table(table),
    )
    dma = pltpu.SemaphoreType.DMA
    vmem = pl.BlockSpec(memory_space=pltpu.VMEM)
    out = pl.pallas_call(
        functools.partial(exchange_kernel, nband, nplane, lines, early),
        out_shape=jax.ShapeDtypeStruct((thick, count, lanes), jnp.float32),
        in_specs=[vmem] * 6,
        out_specs=vmem,
        scratch_shapes=[
            pltpu.VMEM((SOURCES, thick, count, lanes), jnp.float32),
            pltpu.VMEM((thick, nplane, padded, lanes), jnp.float32),
            pltpu.VMEM((count, padded, lanes), jnp.float32),
            pltpu.VMEM((thick, nplane, padded, lanes), jnp.float32),
            dma((2, thick)),
            dma((2, thick)),
            dma((thick,)),
            dma((nplane - 1, thick)),
            dma((nplane - 1, thick)),
            dma((thick,)),
            dma((nplane - 1, thick + 1)),
            dma((nplane - 1, thick + 1)),
            dma((thick + 1,)),
        ],
        compiler_params=pltpu.CompilerParams(
            collective_id=0, has_side_effects=True, vmem_limit_bytes=48 * 2**20
        ),
        name="exchange",
    )(local, filters, *[jnp.asarray(t) for t in tables])
    return out[:, :, :count].reshape(rows, thick, flat)


def solution(mesh):
    placed = (P("band", "plane", None),)
    return jax.shard_map(
        on_device, mesh=mesh, in_specs=placed, out_specs=P("band", "plane", None), check_vma=False
    )
```

```python
import functools
import math

import jax
import jax.numpy as jnp
import numpy as np
from jax import lax
from jax.experimental import pallas as pl
from jax.experimental.pallas import tpu as pltpu
from jax.sharding import PartitionSpec as P

SOURCES = 2
AHEAD = 4

screen_omega = 0.106
cell_length = 46.93
mixing = 0.25


def kernel_values(squares):
    gsquare = squares * (2.0 * math.pi / cell_length) ** 2
    safe = jnp.where(gsquare > 0, gsquare, 1.0)
    values = 4.0 * math.pi / safe * (1.0 - jnp.exp(-safe / (4.0 * screen_omega * screen_omega)))
    return jnp.where(gsquare > 0, values, math.pi / (screen_omega * screen_omega))


def real_basis(count):
    half = count // 2
    freq = np.array(list(range(half + 1)) + list(range(1, count - half)))
    angle = 2.0 * np.pi * (np.arange(count)[:, None] * freq[None, :] % count) / count
    table = np.where(np.arange(count)[None, :] <= half, np.cos(angle), np.sin(angle))
    table = table / np.sqrt((table**2).sum(axis=0, keepdims=True))
    return table.astype(np.float32), freq.astype(np.float32)


MESH = pl.DeviceIdType.MESH


def rounded(value, unit):
    return -(-value // unit) * unit


def high_low(table):
    high = table.astype(jnp.bfloat16)
    low = (table - high.astype(np.float32)).astype(jnp.bfloat16)
    return high, low


def right_table(table, lanes):
    count = table.shape[0]
    high, low = high_low(table)
    out = np.zeros((2 * lanes, 2 * lanes), jnp.bfloat16)
    out[:count, :count] = high
    out[lanes : lanes + count, :count] = high
    out[:count, lanes : lanes + count] = low
    return out


def left_table(table):
    return np.concatenate(high_low(table), axis=0)


def split(values):
    high = values.astype(jnp.bfloat16)
    low = (values - high.astype(jnp.float32)).astype(jnp.bfloat16)
    return jnp.concatenate([high, low], axis=-1)


def from_right(values, table):
    lanes = values.shape[-1]
    out = jnp.dot(split(values), table, preferred_element_type=jnp.float32)
    return out[:, :lanes] + out[:, lanes:]


def from_left(table, values):
    count, lanes = values.shape
    out = jnp.dot(table, split(values), preferred_element_type=jnp.float32)
    return out[:count, :lanes] + (out[:count, lanes:] + out[count:, :lanes])


def run_offsets(count):
    runs = 128 // math.gcd(count, 128)
    return runs, [divmod(u * count, 128) for u in range(runs)]


def exchange_kernel(
    nband, nplane, lines, early,
    flat_ref, right_fwd_ref, right_inv_ref, left_fwd_ref, left_inv_ref, out_ref,
    psi_ref, filter_ref, src_ref, send_ref, full_ref, back_ref,
    spread_send, spread_recv, own_sem, fwd_send, fwd_recv, fwd_own, back_send, back_recv, back_own,
):
    me = lax.axis_index("band")
    here = lax.axis_index("plane")
    mine = lax.rem(me, SOURCES)
    partner = me + 1 - 2 * mine
    above = lax.rem(me + 2, nband)
    below = lax.rem(me + nband - 2, nband)
    thick, count, lanes = psi_ref.shape
    padded = full_ref.shape[1]

    runs, offsets = run_offsets(count)
    psi_rows = psi_ref.reshape(thick * count, lanes)

    def psi_at(y):
        return (pl.ds(y, thick, stride=count), slice(None))

    barrier = pltpu.get_barrier_semaphore()
    for other in (partner, above, below):
        pl.semaphore_signal(barrier, inc=1, device_id={"band": other}, device_id_type=MESH)
    for step in range(1, nplane):
        pl.semaphore_signal(
            barrier, inc=1, device_id={"plane": lax.rem(here + step, nplane)}, device_id_type=MESH
        )

    @pl.loop(0, count // runs)
    def _(t):
        block = flat_ref[:, pl.ds(pl.multiple_of(t * runs * count, 128), runs * count)]
        for u, (tile, shift) in enumerate(offsets):
            wide = block[:, tile * 128 : min((tile + 2) * 128, runs * count)]
            if shift:
                wide = pltpu.roll(wide, wide.shape[1] - shift, 1)
            psi_rows[psi_at(t * runs + u)] = wide[:, :lanes]

    pl.semaphore_wait(barrier, 2 + nplane)

    def own(c):
        return pltpu.make_async_copy(psi_ref.at[c], src_ref.at[mine, c], own_sem.at[c])

    def spread(kind, which, c, target, first=False):
        return pltpu.make_async_remote_copy(
            src_ref=psi_ref.at[c] if first else src_ref.at[which, c],
            dst_ref=src_ref.at[which, c],
            send_sem=spread_send.at[kind, c],
            recv_sem=spread_recv.at[kind, c],
            device_id={"band": target},
            device_id_type=MESH,
        )

    def forward(step, c):
        target = lax.rem(here + step, nplane)
        return pltpu.make_async_remote_copy(
            src_ref=send_ref.at[c, target],
            dst_ref=full_ref.at[here * thick + c],
            send_sem=fwd_send.at[step - 1, c],
            recv_sem=fwd_recv.at[step - 1, c],
            device_id={"plane": target},
            device_id_type=MESH,
        )

    def forward_own(c):
        return pltpu.make_async_copy(
            send_ref.at[c, here], full_ref.at[here * thick + c], fwd_own.at[c]
        )

    def back_parts(c, target):
        if c is None:
            planes, rows = pl.ds(0, thick), pl.ds(0, early)
            source = full_ref.at[pl.ds(target * thick, thick), rows]
            return source, back_ref.at[planes, here, rows], thick
        rows = pl.ds(early, padded - early)
        return full_ref.at[target * thick + c, rows], back_ref.at[c, here, rows], c

    def backward(step, c):
        target = lax.rem(here + step, nplane)
        source, landing, slot = back_parts(c, target)
        return pltpu.make_async_remote_copy(
            src_ref=source,
            dst_ref=landing,
            send_sem=back_send.at[step - 1, slot],
            recv_sem=back_recv.at[step - 1, slot],
            device_id={"plane": target},
            device_id_type=MESH,
        )

    def backward_own(c):
        source, landing, slot = back_parts(c, here)
        return pltpu.make_async_copy(source, landing, back_own.at[slot])

    @pl.when(me < SOURCES)
    def _():
        @pl.loop(0, thick)
        def _(c):
            spread(0, mine, c, above, True).start()
            spread(1, mine, c, partner, True).start()
            own(c).start()

    half_count = count // 2

    def squared(index):
        wave = jnp.where(index <= half_count, index, index - half_count)
        return wave * wave

    plane_squares = squared(lax.broadcasted_iota(jnp.int32, (count, lanes), 0)) + squared(
        lax.broadcasted_iota(jnp.int32, (count, lanes), 1)
    )

    @pl.loop(0, lines)
    def _(r):
        row = squared(lax.rem(here * lines + r, count))
        filter_ref[r] = kernel_values((plane_squares + row).astype(jnp.float32))

    def relay(c):
        @pl.when(me >= SOURCES)
        def _():
            spread(0, mine, c, above).wait_recv()

            @pl.when(me + 2 < nband)
            def _():
                spread(0, mine, c, above).start()

            spread(1, mine, c, partner).start()

    ahead = min(AHEAD, thick)
    for c in range(ahead):
        relay(c)

    @pl.loop(0, thick)
    def _(c):
        @pl.when(c + ahead < thick)
        def _():
            relay(c + ahead)

        @pl.when(me < SOURCES)
        def _():
            own(c).wait()

        spread(1, 1 - mine, c, partner).wait_recv()

        psi = psi_ref[c]
        density = jnp.concatenate([psi * src_ref[j, c] for j in range(SOURCES)], axis=0)
        half = from_right(density, right_fwd_ref[...])
        whole = jnp.concatenate(
            [
                from_left(left_fwd_ref[...], half[j * count : (j + 1) * count])
                for j in range(SOURCES)
            ],
            axis=0,
        )
        for p in range(nplane):
            send_ref[c, p, 0:lines] = whole[p * lines : (p + 1) * lines]
        for step in range(1, nplane):
            forward(step, c).start()
        forward_own(c).start()

    @pl.loop(0, thick)
    def _(c):
        for step in range(1, nplane):
            forward(step, c).wait_recv()
        forward_own(c).wait()

    @pl.loop(0, thick)
    def _(c):
        spread(1, mine, c, partner).wait_send()

        @pl.when(me + 2 < nband)
        def _():
            spread(0, mine, c, above).wait_send()

    rows_ref = full_ref.reshape(nplane * thick * padded, lanes)

    def filtered(r):
        where = (pl.ds(r, count, stride=padded), slice(None))
        spectrum = from_left(left_fwd_ref[...], rows_ref[where]) * filter_ref[r]
        rows_ref[where] = from_left(left_inv_ref[...], spectrum)

    def filter_rows(start, stop):
        unroll = 4 if (stop - start) % 4 == 0 else 2 if (stop - start) % 2 == 0 else 1

        @pl.loop(0, (stop - start) // unroll)
        def _(t):
            for u in range(unroll):
                filtered(start + t * unroll + u)

    if early:
        filter_rows(0, early)
        for step in range(1, nplane):
            backward(step, None).start()
        backward_own(None).start()
    filter_rows(early, lines)

    @pl.loop(0, thick)
    def _(c):
        for step in range(1, nplane):
            backward(step, c).start()
        backward_own(c).start()

    if early:
        for step in range(1, nplane):
            backward(step, None).wait_recv()
        backward_own(None).wait()

    @pl.loop(0, thick)
    def _(c):
        for step in range(1, nplane):
            backward(step, c).wait_recv()
        backward_own(c).wait()
        whole = jnp.concatenate([back_ref[c, p, 0:lines] for p in range(nplane)], axis=0)
        half = jnp.concatenate(
            [
                from_left(left_inv_ref[...], whole[j * count : (j + 1) * count])
                for j in range(SOURCES)
            ],
            axis=0,
        )
        potential = from_right(half, right_inv_ref[...])
        total = src_ref[0, c] * potential[:count]
        for j in range(1, SOURCES):
            total = total + src_ref[j, c] * potential[j * count : (j + 1) * count]
        psi_ref[c] = -mixing * total

    @pl.loop(0, thick)
    def _(c):
        for step in range(1, nplane):
            forward(step, c).wait_send()
            backward(step, c).wait_send()

    if early:
        for step in range(1, nplane):
            backward(step, None).wait_send()

    @pl.loop(0, count // runs)
    def _(t):
        tiles = [None] * (runs * count // 128)
        for u, (tile, shift) in enumerate(offsets):
            value = psi_rows[psi_at(t * runs + u)]
            if not shift:
                parts = [value]
            else:
                wide = jnp.concatenate([value, jnp.zeros_like(value)], axis=1)
                wide = pltpu.roll(wide, shift, 1)
                parts = [wide[:, :128], wide[:, 128:]]
            for k, piece in enumerate(parts):
                if tile + k < len(tiles):
                    old = tiles[tile + k]
                    tiles[tile + k] = piece if old is None else old + piece
        out_ref[:, pl.ds(pl.multiple_of(t * runs * count, 128), runs * count)] = jnp.concatenate(
            tiles, axis=1
        )


def on_device(orbitals):
    nband = lax.axis_size("band")
    nplane = lax.axis_size("plane")
    rows, thick, flat = orbitals.shape
    count = thick * nplane
    lanes = rounded(count, 128)
    lines = SOURCES * count // nplane
    padded = rounded(lines, 8)
    early = 16 if padded >= 32 else 8 if padded >= 16 else 0
    table, _ = real_basis(count)
    tables = (
        right_table(table, lanes),
        right_table(table.T, lanes),
        left_table(table.T),
        left_table(table),
    )
    dma = pltpu.SemaphoreType.DMA
    vmem = pl.BlockSpec(memory_space=pltpu.VMEM)
    out = pl.pallas_call(
        functools.partial(exchange_kernel, nband, nplane, lines, early),
        out_shape=jax.ShapeDtypeStruct((thick, flat), jnp.float32),
        in_specs=[vmem] * 5,
        out_specs=vmem,
        scratch_shapes=[
            pltpu.VMEM((thick, count, lanes), jnp.float32),
            pltpu.VMEM((lines, count, lanes), jnp.float32),
            pltpu.VMEM((SOURCES, thick, count, lanes), jnp.float32),
            pltpu.VMEM((thick, nplane, padded, lanes), jnp.float32),
            pltpu.VMEM((count, padded, lanes), jnp.float32),
            pltpu.VMEM((thick, nplane, padded, lanes), jnp.float32),
            dma((2, thick)),
            dma((2, thick)),
            dma((thick,)),
            dma((nplane - 1, thick)),
            dma((nplane - 1, thick)),
            dma((thick,)),
            dma((nplane - 1, thick + 1)),
            dma((nplane - 1, thick + 1)),
            dma((thick + 1,)),
        ],
        compiler_params=pltpu.CompilerParams(
            collective_id=0, has_side_effects=True, vmem_limit_bytes=48 * 2**20
        ),
        name="exchange",
    )(orbitals.reshape(thick, flat), *[jnp.asarray(t) for t in tables])
    return out.reshape(rows, thick, flat)


def solution(mesh):
    placed = (P("band", "plane", None),)
    return jax.shard_map(
        on_device, mesh=mesh, in_specs=placed, out_specs=P("band", "plane", None), check_vma=False
    )
```

```python
import functools
import math

import jax
import jax.numpy as jnp
import numpy as np
from jax import lax
from jax.experimental import pallas as pl
from jax.experimental.pallas import tpu as pltpu
from jax.sharding import PartitionSpec as P

SOURCES = 2
AHEAD = 2

screen_omega = 0.106
cell_length = 46.93
mixing = 0.25


def kernel_values(squares):
    gsquare = squares * (2.0 * math.pi / cell_length) ** 2
    safe = jnp.where(gsquare > 0, gsquare, 1.0)
    values = 4.0 * math.pi / safe * (1.0 - jnp.exp(-safe / (4.0 * screen_omega * screen_omega)))
    return jnp.where(gsquare > 0, values, math.pi / (screen_omega * screen_omega))


def real_basis(count):
    half = count // 2
    freq = np.array(list(range(half + 1)) + list(range(1, count - half)))
    angle = 2.0 * np.pi * (np.arange(count)[:, None] * freq[None, :] % count) / count
    table = np.where(np.arange(count)[None, :] <= half, np.cos(angle), np.sin(angle))
    table = table / np.sqrt((table**2).sum(axis=0, keepdims=True))
    return table.astype(np.float32), freq.astype(np.float32)


MESH = pl.DeviceIdType.MESH


def rounded(value, unit):
    return -(-value // unit) * unit


def high_low(table):
    high = table.astype(jnp.bfloat16)
    low = (table - high.astype(np.float32)).astype(jnp.bfloat16)
    return high, low


def right_table(table, lanes):
    count = table.shape[0]
    high, low = high_low(table)
    out = np.zeros((2 * lanes, 2 * lanes), jnp.bfloat16)
    out[:count, :count] = high
    out[lanes : lanes + count, :count] = high
    out[:count, lanes : lanes + count] = low
    return out


def left_table(table):
    return np.concatenate(high_low(table), axis=0)


def split(values):
    high = values.astype(jnp.bfloat16)
    low = (values - high.astype(jnp.float32)).astype(jnp.bfloat16)
    return jnp.concatenate([high, low], axis=-1)


def from_right(values, table):
    lanes = values.shape[-1]
    out = jnp.dot(split(values), table, preferred_element_type=jnp.float32)
    return out[:, :lanes] + out[:, lanes:]


def from_left(table, values):
    count, lanes = values.shape
    out = jnp.dot(table, split(values), preferred_element_type=jnp.float32)
    return out[:count, :lanes] + (out[:count, lanes:] + out[count:, :lanes])


def run_offsets(count):
    runs = 128 // math.gcd(count, 128)
    return runs, [divmod(u * count, 128) for u in range(runs)]


def exchange_kernel(
    nband, nplane, lines, early,
    flat_ref, right_fwd_ref, right_inv_ref, left_fwd_ref, left_inv_ref, out_ref,
    psi_ref, filter_ref, src_ref, send_ref, full_ref, back_ref,
    spread_send, spread_recv, own_sem, fwd_send, fwd_recv, fwd_own, back_send, back_recv, back_own,
):
    me = lax.axis_index("band")
    here = lax.axis_index("plane")
    mine = lax.rem(me, SOURCES)
    partner = me + 1 - 2 * mine
    above = lax.rem(me + 2, nband)
    below = lax.rem(me + nband - 2, nband)
    thick, count, lanes = psi_ref.shape
    padded = full_ref.shape[1]

    runs, offsets = run_offsets(count)
    psi_rows = psi_ref.reshape(thick * count, lanes)

    def psi_at(y):
        return (pl.ds(y, thick, stride=count), slice(None))

    barrier = pltpu.get_barrier_semaphore()
    for other in (partner, above, below):
        pl.semaphore_signal(barrier, inc=1, device_id={"band": other}, device_id_type=MESH)
    for step in range(1, nplane):
        pl.semaphore_signal(
            barrier, inc=1, device_id={"plane": lax.rem(here + step, nplane)}, device_id_type=MESH
        )

    @pl.loop(0, count // runs)
    def _(t):
        block = flat_ref[:, pl.ds(pl.multiple_of(t * runs * count, 128), runs * count)]
        for u, (tile, shift) in enumerate(offsets):
            wide = block[:, tile * 128 : min((tile + 2) * 128, runs * count)]
            if shift:
                wide = pltpu.roll(wide, wide.shape[1] - shift, 1)
            psi_rows[psi_at(t * runs + u)] = wide[:, :lanes]

    pl.semaphore_wait(barrier, 2 + nplane)

    def own(c):
        return pltpu.make_async_copy(psi_ref.at[c], src_ref.at[mine, c], own_sem.at[c])

    def spread(kind, which, c, target, first=False):
        return pltpu.make_async_remote_copy(
            src_ref=psi_ref.at[c] if first else src_ref.at[which, c],
            dst_ref=src_ref.at[which, c],
            send_sem=spread_send.at[kind, c],
            recv_sem=spread_recv.at[kind, c],
            device_id={"band": target},
            device_id_type=MESH,
        )

    def forward(step, c):
        target = lax.rem(here + step, nplane)
        return pltpu.make_async_remote_copy(
            src_ref=send_ref.at[c, target],
            dst_ref=full_ref.at[here * thick + c],
            send_sem=fwd_send.at[step - 1, c],
            recv_sem=fwd_recv.at[step - 1, c],
            device_id={"plane": target},
            device_id_type=MESH,
        )

    def forward_own(c):
        return pltpu.make_async_copy(
            send_ref.at[c, here], full_ref.at[here * thick + c], fwd_own.at[c]
        )

    def back_parts(c, target):
        if c is None:
            planes, rows = pl.ds(0, thick), pl.ds(0, early)
            source = full_ref.at[pl.ds(target * thick, thick), rows]
            return source, back_ref.at[planes, here, rows], thick
        rows = pl.ds(early, padded - early)
        return full_ref.at[target * thick + c, rows], back_ref.at[c, here, rows], c

    def backward(step, c):
        target = lax.rem(here + step, nplane)
        source, landing, slot = back_parts(c, target)
        return pltpu.make_async_remote_copy(
            src_ref=source,
            dst_ref=landing,
            send_sem=back_send.at[step - 1, slot],
            recv_sem=back_recv.at[step - 1, slot],
            device_id={"plane": target},
            device_id_type=MESH,
        )

    def backward_own(c):
        source, landing, slot = back_parts(c, here)
        return pltpu.make_async_copy(source, landing, back_own.at[slot])

    @pl.when(me < SOURCES)
    def _():
        @pl.loop(0, thick)
        def _(c):
            spread(0, mine, c, above, True).start()
            spread(1, mine, c, partner, True).start()
            own(c).start()

    half_count = count // 2

    def squared(index):
        wave = jnp.where(index <= half_count, index, index - half_count)
        return wave * wave

    plane_squares = squared(lax.broadcasted_iota(jnp.int32, (count, lanes), 0)) + squared(
        lax.broadcasted_iota(jnp.int32, (count, lanes), 1)
    )

    @pl.loop(0, lines)
    def _(r):
        row = squared(lax.rem(here * lines + r, count))
        filter_ref[r] = kernel_values((plane_squares + row).astype(jnp.float32))

    def relay(c):
        @pl.when(me >= SOURCES)
        def _():
            spread(0, mine, c, above).wait_recv()

            @pl.when(me + 2 < nband)
            def _():
                spread(0, mine, c, above).start()

            spread(1, mine, c, partner).start()

    ahead = min(AHEAD, thick)
    for c in range(ahead):
        relay(c)

    @pl.loop(0, thick)
    def _(c):
        @pl.when(c + ahead < thick)
        def _():
            relay(c + ahead)

        @pl.when(me < SOURCES)
        def _():
            own(c).wait()

        spread(1, 1 - mine, c, partner).wait_recv()

        psi = psi_ref[c]
        density = jnp.concatenate([psi * src_ref[j, c] for j in range(SOURCES)], axis=0)
        half = from_right(density, right_fwd_ref[...])
        whole = jnp.concatenate(
            [
                from_left(left_fwd_ref[...], half[j * count : (j + 1) * count])
                for j in range(SOURCES)
            ],
            axis=0,
        )
        for p in range(nplane):
            send_ref[c, p, 0:lines] = whole[p * lines : (p + 1) * lines]
        for step in range(1, nplane):
            forward(step, c).start()
        forward_own(c).start()

    @pl.loop(0, thick)
    def _(c):
        for step in range(1, nplane):
            forward(step, c).wait_recv()
        forward_own(c).wait()

    @pl.loop(0, thick)
    def _(c):
        spread(1, mine, c, partner).wait_send()

        @pl.when(me + 2 < nband)
        def _():
            spread(0, mine, c, above).wait_send()

    rows_ref = full_ref.reshape(nplane * thick * padded, lanes)

    def filtered(r):
        where = (pl.ds(r, count, stride=padded), slice(None))
        spectrum = from_left(left_fwd_ref[...], rows_ref[where]) * filter_ref[r]
        rows_ref[where] = from_left(left_inv_ref[...], spectrum)

    def filter_rows(start, stop):
        unroll = 4 if (stop - start) % 4 == 0 else 2 if (stop - start) % 2 == 0 else 1

        @pl.loop(0, (stop - start) // unroll)
        def _(t):
            for u in range(unroll):
                filtered(start + t * unroll + u)

    if early:
        filter_rows(0, early)
        for step in range(1, nplane):
            backward(step, None).start()
        backward_own(None).start()
    filter_rows(early, lines)

    @pl.loop(0, thick)
    def _(c):
        for step in range(1, nplane):
            backward(step, c).start()
        backward_own(c).start()

    if early:
        for step in range(1, nplane):
            backward(step, None).wait_recv()
        backward_own(None).wait()

    @pl.loop(0, thick)
    def _(c):
        for step in range(1, nplane):
            backward(step, c).wait_recv()
        backward_own(c).wait()
        whole = jnp.concatenate([back_ref[c, p, 0:lines] for p in range(nplane)], axis=0)
        half = jnp.concatenate(
            [
                from_left(left_inv_ref[...], whole[j * count : (j + 1) * count])
                for j in range(SOURCES)
            ],
            axis=0,
        )
        potential = from_right(half, right_inv_ref[...])
        total = src_ref[0, c] * potential[:count]
        for j in range(1, SOURCES):
            total = total + src_ref[j, c] * potential[j * count : (j + 1) * count]
        psi_ref[c] = -mixing * total

    @pl.loop(0, thick)
    def _(c):
        for step in range(1, nplane):
            forward(step, c).wait_send()
            backward(step, c).wait_send()

    if early:
        for step in range(1, nplane):
            backward(step, None).wait_send()

    @pl.loop(0, count // runs)
    def _(t):
        tiles = [None] * (runs * count // 128)
        for u, (tile, shift) in enumerate(offsets):
            value = psi_rows[psi_at(t * runs + u)]
            if not shift:
                parts = [value]
            else:
                wide = jnp.concatenate([value, jnp.zeros_like(value)], axis=1)
                wide = pltpu.roll(wide, shift, 1)
                parts = [wide[:, :128], wide[:, 128:]]
            for k, piece in enumerate(parts):
                if tile + k < len(tiles):
                    old = tiles[tile + k]
                    tiles[tile + k] = piece if old is None else old + piece
        out_ref[:, pl.ds(pl.multiple_of(t * runs * count, 128), runs * count)] = jnp.concatenate(
            tiles, axis=1
        )


def on_device(orbitals):
    nband = lax.axis_size("band")
    nplane = lax.axis_size("plane")
    rows, thick, flat = orbitals.shape
    count = thick * nplane
    lanes = rounded(count, 128)
    lines = SOURCES * count // nplane
    padded = rounded(lines, 8)
    early = 8 if padded >= 16 else 0
    table, _ = real_basis(count)
    tables = (
        right_table(table, lanes),
        right_table(table.T, lanes),
        left_table(table.T),
        left_table(table),
    )
    dma = pltpu.SemaphoreType.DMA
    vmem = pl.BlockSpec(memory_space=pltpu.VMEM)
    out = pl.pallas_call(
        functools.partial(exchange_kernel, nband, nplane, lines, early),
        out_shape=jax.ShapeDtypeStruct((thick, flat), jnp.float32),
        in_specs=[vmem] * 5,
        out_specs=vmem,
        scratch_shapes=[
            pltpu.VMEM((thick, count, lanes), jnp.float32),
            pltpu.VMEM((lines, count, lanes), jnp.float32),
            pltpu.VMEM((SOURCES, thick, count, lanes), jnp.float32),
            pltpu.VMEM((thick, nplane, padded, lanes), jnp.float32),
            pltpu.VMEM((count, padded, lanes), jnp.float32),
            pltpu.VMEM((thick, nplane, padded, lanes), jnp.float32),
            dma((2, thick)),
            dma((2, thick)),
            dma((thick,)),
            dma((nplane - 1, thick)),
            dma((nplane - 1, thick)),
            dma((thick,)),
            dma((nplane - 1, thick + 1)),
            dma((nplane - 1, thick + 1)),
            dma((thick + 1,)),
        ],
        compiler_params=pltpu.CompilerParams(
            collective_id=0, has_side_effects=True, vmem_limit_bytes=48 * 2**20
        ),
        name="exchange",
    )(orbitals.reshape(thick, flat), *[jnp.asarray(t) for t in tables])
    return out.reshape(rows, thick, flat)


def solution(mesh):
    placed = (P("band", "plane", None),)
    return jax.shard_map(
        on_device, mesh=mesh, in_specs=placed, out_specs=P("band", "plane", None), check_vma=False
    )
```
